32 devices in a mesh: px: 4 (over z), py: 8 (over y, x, core).
Axes of the slice: x: 2, y: 2, z: 4, core: 2. Of those that a mesh axis runs over, the one named last changes fastest.
Arguments:
- latents: float32 [16, 64, 48, 768], P('px', None, 'py'), may hold values from -6 to 6
- norm1_gain: float32 [768], replicated, may hold values from 0.1 to 1.9
- norm1_shift: float32 [768], replicated, may hold values from -3 to 3
- spectral_in: float32 [2, 8, 96, 96], P(None, 'px'), may hold values from -0.4375 to 0.4375
- spectral_in_bias: float32 [2, 8, 96], P(None, 'px'), may hold values from -3 to 3
- spectral_out: float32 [2, 8, 96, 96], P(None, 'px'), may hold values from -0.4375 to 0.4375
- spectral_out_bias: float32 [2, 8, 96], P(None, 'px'), may hold values from -3 to 3
- norm2_gain: float32 [768], replicated, may hold values from 0.1 to 1.9
- norm2_shift: float32 [768], replicated, may hold values from -3 to 3
- fc_in: bfloat16 [768, 3072], replicated, may hold values from -0.21875 to 0.21875
- fc_in_bias: float32 [3072], replicated, may hold values from -3 to 3
- fc_out: bfloat16 [3072, 768], replicated, may hold values from -0.109375 to 0.109375
- fc_out_bias: float32 [768], replicated, may hold values from -3 to 3
Outputs:
- result: float32 [16, 64, 48, 768], P('px', None, 'py')
The draws below stay inside these ranges and needn't reach their ends.
All inputs are finite; a program needn't handle non-finite values.
Results may differ from the reference program's by a relative error of at most 0.0014.
Values sent between devices are 32-bit elements; how exact they have to be, the bound alone decides.
No kernel may reach another device: no remote copies, remote signals or barrier semaphores. Data moves between devices by JAX's collectives and lax.ppermute only.
A program may use at most 128 MiB of HBM per device.

```python
import jax
import jax.numpy as jnp
from jax import lax

F = 16
H = 64
W = 48
C = 768
BLOCKS = 8
FF = 3072
BLOCK = 96


def shard_levels(own_key, extent, pieces, least, high):
    def one(axis_at, shards_of):
        steps = jax.random.uniform(jax.random.fold_in(jax.random.fold_in(own_key, 6), axis_at), (shards_of,), jnp.float32, least / len(pieces), high / len(pieces))
        return jnp.repeat(jnp.exp(steps), extent[axis_at] // shards_of).reshape((-1,) + (1,) * (len(extent) - axis_at - 1))

    level = one(*pieces[0])
    for cut in pieces[1:]:
        level = level * one(*cut)
    return level


def noise(own_key, extent, spread, bound, pieces=(), kind=jnp.bfloat16):
    drawn = jax.random.normal(own_key, extent, jnp.float32) * spread
    if len(pieces) > 0:
        drawn = shard_levels(own_key, extent, pieces, -0.22, 0.18) * drawn
    return jnp.clip(drawn, min=-bound, max=bound).astype(kind)


def setup_inputs(seed: int = 0) -> dict:
    arg_keys = jax.random.split(jax.random.key(seed), 14)
    return {
        "latents": noise(arg_keys[0], (F, H, W, C), 1.0, 6.0, ((0, 4), (2, 8)), jnp.float32),
        "norm1_gain": jnp.clip(1.0 + 0.18 * jax.random.normal(arg_keys[1], (C,), jnp.float32), 0.1, 1.9),
        "norm1_shift": noise(arg_keys[2], (C,), 0.5, 3.0, (), jnp.float32),
        "spectral_in": noise(arg_keys[3], (2, BLOCKS, BLOCK, BLOCK), (2 * BLOCK) ** -0.5, 0.4375, ((1, 4),), jnp.float32),
        "spectral_in_bias": noise(arg_keys[4], (2, BLOCKS, BLOCK), 0.5, 3.0, ((1, 4),), jnp.float32),
        "spectral_out": noise(arg_keys[5], (2, BLOCKS, BLOCK, BLOCK), (2 * BLOCK) ** -0.5, 0.4375, ((1, 4),), jnp.float32),
        "spectral_out_bias": noise(arg_keys[6], (2, BLOCKS, BLOCK), 0.5, 3.0, ((1, 4),), jnp.float32),
        "norm2_gain": jnp.clip(1.0 + 0.18 * jax.random.normal(arg_keys[7], (C,), jnp.float32), 0.1, 1.9),
        "norm2_shift": noise(arg_keys[8], (C,), 0.5, 3.0, (), jnp.float32),
        "fc_in": noise(arg_keys[9], (C, FF), C ** -0.5, 0.21875),
        "fc_in_bias": noise(arg_keys[10], (FF,), 0.5, 3.0, (), jnp.float32),
        "fc_out": noise(arg_keys[11], (FF, C), FF ** -0.5, 0.109375),
        "fc_out_bias": noise(arg_keys[12], (C,), 0.5, 3.0, (), jnp.float32),
    }


HIGH = lax.Precision.HIGHEST

def layer_norm(values, gain, shift):
    mean = lax.optimization_barrier(jnp.mean(values, axis=-1, keepdims=True))
    centred = values - mean
    variance = lax.optimization_barrier(jnp.mean(centred * centred, axis=-1, keepdims=True))
    return centred / jnp.sqrt(variance + 1e-05) * gain + shift

def block_dense(real_part, imag_part, weight, bias):
    out_real = jnp.einsum('hwbi,bio->hwbo', real_part, weight[0], precision=HIGH) - jnp.einsum('hwbi,bio->hwbo', imag_part, weight[1], precision=HIGH) + bias[0]
    out_imag = jnp.einsum('hwbi,bio->hwbo', imag_part, weight[0], precision=HIGH) + jnp.einsum('hwbi,bio->hwbo', real_part, weight[1], precision=HIGH) + bias[1]
    return (out_real, out_imag)

def shrink(values):
    return jnp.maximum(values - 0.1, 0.0) + jnp.minimum(values + 0.1, 0.0)

def reference(latents, norm1_gain, norm1_shift, spectral_in, spectral_in_bias, spectral_out, spectral_out_bias, norm2_gain, norm2_shift, fc_in, fc_in_bias, fc_out, fc_out_bias):
    normed = layer_norm(latents, norm1_gain, norm1_shift)
    spectrum = jnp.fft.fftn(normed, axes=(0, 1, 2), norm='ortho')
    spec_real = jnp.real(spectrum).reshape(F, H, W, BLOCKS, BLOCK)
    spec_imag = jnp.imag(spectrum).reshape(F, H, W, BLOCKS, BLOCK)

    def per_frame(frame):
        real_part, imag_part = frame
        first_real, first_imag = block_dense(real_part, imag_part, spectral_in, spectral_in_bias)
        first_real = jnp.maximum(first_real, 0.0)
        first_imag = jnp.maximum(first_imag, 0.0)
        second_real, second_imag = block_dense(first_real, first_imag, spectral_out, spectral_out_bias)
        return (shrink(second_real), shrink(second_imag))
    filt_real, filt_imag = lax.map(per_frame, (spec_real, spec_imag))
    filtered = lax.complex(filt_real.reshape(F, H, W, C), filt_imag.reshape(F, H, W, C))
    mixed = jnp.real(jnp.fft.ifftn(filtered, axes=(0, 1, 2), norm='ortho'))
    after_mix = latents + mixed + normed

    def channel_mlp(frame):
        rows = frame.reshape(H * W, C)
        normed2 = layer_norm(rows, norm2_gain, norm2_shift).astype(jnp.bfloat16)
        hidden = jax.nn.gelu(jnp.dot(normed2, fc_in, preferred_element_type=jnp.float32) + fc_in_bias).astype(jnp.bfloat16)
        output = rows + jnp.dot(hidden, fc_out, preferred_element_type=jnp.float32) + fc_out_bias
        return output.reshape(H, W, C)
    return lax.map(channel_mlp, after_mix)
```

```python
import functools
import math

import numpy as np

import jax
import jax.numpy as jnp
from jax import lax
from jax.experimental import pallas as pl
from jax.experimental.pallas import tpu as pltpu
from jax.sharding import PartitionSpec as P


F32 = jnp.float32
BF16 = jnp.bfloat16
LANES = 128
SUB = 8
CHUNKS = 4


def cmul_const(value, re, im):
    a, b = value
    if abs(im) < 1e-12:
        if abs(re - 1.0) < 1e-12:
            return value
        if abs(re + 1.0) < 1e-12:
            return (-a, -b)
        return (a * re, b * re)
    if abs(re) < 1e-12:
        if abs(im - 1.0) < 1e-12:
            return (-b, a)
        if abs(im + 1.0) < 1e-12:
            return (b, -a)
        return (b * -im, a * im)
    return (a * re - b * im, a * im + b * re)


def cadd(x, y):
    return (x[0] + y[0], x[1] + y[1])


def csub(x, y):
    return (x[0] - y[0], x[1] - y[1])


def fft(values, sign):
    n = len(values)
    if n == 1:
        return values
    if n % 2 == 0:
        half = n // 2
        even, odd = fft(values[0::2], sign), fft(values[1::2], sign)
        out = [None] * n
        for k in range(half):
            angle = sign * 2.0 * math.pi * k / n
            turned = cmul_const(odd[k], math.cos(angle), math.sin(angle))
            out[k] = cadd(even[k], turned)
            out[k + half] = csub(even[k], turned)
        return out
    radix = next(r for r in range(3, n + 1) if n % r == 0)
    part = n // radix
    subs = [fft(values[r::radix], sign) for r in range(radix)]
    out = [None] * n
    for k in range(part):
        turned = []
        for r in range(radix):
            angle = sign * 2.0 * math.pi * k * r / n
            turned.append(cmul_const(subs[r][k], math.cos(angle), math.sin(angle)))
        if radix == 3:
            total = cadd(turned[1], turned[2])
            apart = csub(turned[1], turned[2])
            out[k] = cadd(turned[0], total)
            mid = (turned[0][0] - 0.5 * total[0], turned[0][1] - 0.5 * total[1])
            s = sign * math.sqrt(3.0) / 2.0
            side = (-s * apart[1], s * apart[0])
            out[k + part] = cadd(mid, side)
            out[k + 2 * part] = csub(mid, side)
        else:
            for t in range(radix):
                acc = turned[0]
                for r in range(1, radix):
                    angle = sign * 2.0 * math.pi * r * t / radix
                    acc = cadd(acc, cmul_const(turned[r], math.cos(angle), math.sin(angle)))
                out[k + t * part] = acc
    return out


def split_bf16(values):
    high = values.astype(BF16)
    return high, (values - high.astype(F32)).astype(BF16)


def split_outside(values):
    high = lax.reduce_precision(values, exponent_bits=8, mantissa_bits=7)
    return high.astype(BF16), (values - high).astype(BF16)


def dot32(a, b):
    return jnp.dot(a, b, preferred_element_type=F32)


class Sizes:
    def __init__(self, mesh, latents_shape, spectral_shape):
        self.nx, self.ny = mesh.shape["px"], mesh.shape["py"]
        self.f, self.h, self.wl, self.c = latents_shape
        self.frames, self.w = self.f * self.nx, self.wl * self.ny
        self.groups, self.block = spectral_shape[1], spectral_shape[2]
        self.cl = self.c // self.nx
        self.wg = next((d for d in range(1, self.wl + 1) if self.wl % d == 0 and d * self.cl % LANES == 0), 1)
        self.wp = self.wl // self.wg
        self.lt = -(-self.wg * self.cl // LANES)
        self.pairs = self.h // 2
        self.ns = self.pairs // self.ny
        chunks = max(d for d in range(1, min(CHUNKS, self.ns) + 1) if self.ns % d == 0)
        self.chunks, self.sc = chunks, self.ns // chunks
        self.rows = 2 * self.sc * self.ny
        self.m = self.w // self.wg


def height_tables(z):
    n = np.arange(z.h)
    scale = 1.0 / math.sqrt(z.frames * z.h * z.w)
    forward, inverse = [], []
    for chunk in range(z.chunks):
        for part in range(2):
            for s in range(chunk * z.sc, (chunk + 1) * z.sc):
                for q in range(z.ny):
                    k = s * z.ny + q
                    angle = 2.0 * math.pi * ((k * n) % z.h) / z.h
                    if k == 0:
                        row = np.ones(z.h) if part == 0 else np.cos(math.pi * n)
                        forward.append(row * scale)
                        inverse.append(row * (0.5 * scale))
                    else:
                        row = np.cos(angle) if part == 0 else -np.sin(angle)
                        forward.append(row * scale)
                        inverse.append(row * scale)
    return np.stack(forward).astype(np.float32), np.stack(inverse, axis=1).astype(np.float32)


def stacked3(matrix):
    high = matrix.astype(jnp.bfloat16)
    low = (matrix - high.astype(np.float32)).astype(jnp.bfloat16)
    return np.concatenate([high, high, low], axis=1)


def rhs3(values):
    high, low = split_bf16(values)
    return jnp.concatenate([high, low, high], axis=0)


def k1_body(z, idx_ref, lat_ref, gain_ref, shift_ref, mat_ref, base_ref, *rest):
    outs = rest[: z.chunks * z.nx]
    (blk_scr,) = rest[z.chunks * z.nx :]
    ip = idx_ref[0]
    mat = mat_ref[...]
    for wp in range(z.wp):
        cols = []
        for e in range(z.wg):
            w = wp * z.wg + e
            x = lat_ref[0, w]
            mean = jnp.mean(x, axis=-1, keepdims=True)
            centred = x - mean
            var = jnp.mean(centred * centred, axis=-1, keepdims=True)
            normed = centred / jnp.sqrt(var + 1e-05) * gain_ref[...] + shift_ref[...]
            base_ref[0, w] = x + normed
            cols.append(dot32(mat, rhs3(normed)))
        for p in range(z.nx):
            parts = [y[:, p * z.cl : (p + 1) * z.cl] for y in cols]
            if z.lt * LANES > z.wg * z.cl:
                parts.append(jnp.zeros((z.h, z.lt * LANES - z.wg * z.cl), F32))
            blk = jnp.concatenate(parts, axis=1) if len(parts) > 1 else parts[0]
            for l in range(z.lt):
                blk_scr[p, l] = blk[:, l * LANES : (l + 1) * LANES]
        for c in range(z.chunks):
            for s in range(z.nx):
                p = lax.rem(ip + s, z.nx)
                outs[c * z.nx + s][0, wp] = blk_scr[p, :, c * z.rows : (c + 1) * z.rows, :]


def kernel1(z, idx, latents, gain, shift, matrix):
    const = lambda *shape: pl.BlockSpec(shape, lambda i, _: (0,) * len(shape))
    out_shape = [jax.ShapeDtypeStruct((z.f, z.wl, z.h, z.c), F32)]
    out_specs = [pl.BlockSpec((1, z.wl, z.h, z.c), lambda i, _: (i, 0, 0, 0))]
    for _ in range(z.chunks * z.nx):
        out_shape.append(jax.ShapeDtypeStruct((z.f, z.wp, z.lt, z.rows, LANES), F32))
        out_specs.append(pl.BlockSpec((1, z.wp, z.lt, z.rows, LANES), lambda i, _: (i, 0, 0, 0, 0)))
    outs = pl.pallas_call(
        functools.partial(k1_body, z),
        out_shape=out_shape,
        grid_spec=pltpu.PrefetchScalarGridSpec(
            num_scalar_prefetch=1,
            grid=(z.f,),
            in_specs=[
                pl.BlockSpec((1, z.wl, z.h, z.c), lambda i, _: (i, 0, 0, 0)),
                const(1, z.c),
                const(1, z.c),
                const(z.h, 3 * z.h),
            ],
            out_specs=out_specs,
            scratch_shapes=[
                pltpu.VMEM((z.nx, z.lt, z.h, LANES), F32),
            ],
        ),
        cost_estimate=pl.CostEstimate(flops=2 * 10**9, bytes_accessed=10**7, transcendentals=0),
        name="k1",
    )(idx, latents, gain[None], shift[None], matrix)
    return outs[0], [outs[1 + c * z.nx : 1 + (c + 1) * z.nx] for c in range(z.chunks)]


def k2_body(z, special, idx_ref, *refs):
    ins, outs = refs[: z.nx], refs[z.nx : z.nx + z.ny]
    in_scr, out_scr = refs[z.nx + z.ny :]
    ip, iq = idx_ref[0], idx_ref[1]
    for s in range(z.nx):
        in_scr[lax.rem(ip + z.nx - s, z.nx)] = ins[s][:, 0]
    half = z.frames // 2
    stride = z.sc * 2 * z.lt * z.frames
    flat = out_scr.reshape(z.ny * stride, LANES)
    for s in range(z.sc):
        for qt in range(z.ny // SUB):
            for l in range(z.lt):
                r0 = s * z.ny + qt * SUB
                r1 = z.sc * z.ny + r0
                values = [
                    (in_scr[n // z.f, n % z.f, l, r0 : r0 + SUB, :], in_scr[n // z.f, n % z.f, l, r1 : r1 + SUB, :])
                    for n in range(z.frames)
                ]
                u = fft(values, -1.0)
                if special and s == 0 and qt == 0:
                    first = lax.broadcasted_iota(jnp.int32, (SUB, LANES), 0) == 0
                    sel = lambda x, y: (jnp.where(first, x[0], y[0]), jnp.where(first, x[1], y[1]))
                    v = list(u)
                    v[0] = sel((u[0][0], u[half][0]), u[0])
                    v[half] = sel((u[0][1], u[half][1]), u[half])
                    for k in range(1, half):
                        a, b = u[k], u[z.frames - k]
                        v[k] = sel(((a[0] + b[0]) * 0.5, (a[1] - b[1]) * 0.5), u[k])
                        v[k + half] = sel(((a[1] + b[1]) * 0.5, (b[0] - a[0]) * 0.5), u[k + half])
                    u = v
                for k in range(z.frames):
                    for ri in range(2):
                        row = qt * SUB * stride + ((s * 2 + ri) * z.lt + l) * z.frames + k
                        flat[pl.ds(row, SUB, stride=stride), :] = u[k][ri]
    for s in range(z.ny):
        outs[s][:, :, 0] = out_scr[lax.rem(iq + s, z.ny)]


def kernel2(z, special, idx, arrays):
    in_spec = pl.BlockSpec((z.f, 1, z.lt, z.rows, LANES), lambda i, _: (0, i, 0, 0, 0))
    out_spec = pl.BlockSpec((z.sc, 2, 1, z.lt, z.frames, LANES), lambda i, _: (0, 0, i, 0, 0, 0))
    return pl.pallas_call(
        functools.partial(k2_body, z, special),
        out_shape=[jax.ShapeDtypeStruct((z.sc, 2, z.wp, z.lt, z.frames, LANES), F32)] * z.ny,
        grid_spec=pltpu.PrefetchScalarGridSpec(
            num_scalar_prefetch=1,
            grid=(z.wp,),
            in_specs=[in_spec] * z.nx,
            out_specs=[out_spec] * z.ny,
            scratch_shapes=[
                pltpu.VMEM((z.nx, z.f, z.lt, z.rows, LANES), F32),
                pltpu.VMEM((z.ny, z.sc, 2, z.lt, z.frames, LANES), F32),
            ],
        ),
        cost_estimate=pl.CostEstimate(flops=10**9, bytes_accessed=3 * 10**6, transcendentals=0),
        name="k2",
    )(idx, *arrays)


def k4_body(z, special, idx_ref, *refs):
    ins, outs = refs[: z.ny], refs[z.ny : z.ny + z.nx]
    in_scr, out_scr = refs[z.ny + z.nx :]
    ip, iq = idx_ref[0], idx_ref[1]
    for s in range(z.ny):
        in_scr[lax.rem(iq + z.ny - s, z.ny)] = ins[s][:, :, 0]
    half = z.frames // 2
    stride = z.sc * 2 * z.lt * z.frames
    flat = in_scr.reshape(z.ny * stride, LANES)
    for s in range(z.sc):
        for qt in range(z.ny // SUB):
            for l in range(z.lt):
                v = []
                for k in range(z.frames):
                    rows = [qt * SUB * stride + ((s * 2 + ri) * z.lt + l) * z.frames + k for ri in range(2)]
                    v.append(tuple(flat[pl.ds(row, SUB, stride=stride), :] for row in rows))
                if special and s == 0 and qt == 0:
                    first = lax.broadcasted_iota(jnp.int32, (SUB, LANES), 0) == 0
                    sel = lambda x, y: (jnp.where(first, x[0], y[0]), jnp.where(first, x[1], y[1]))
                    u = list(v)
                    u[0] = sel((v[0][0], v[half][0]), v[0])
                    u[half] = sel((v[0][1], v[half][1]), v[half])
                    for k in range(1, half):
                        a, b = v[k], v[k + half]
                        u[k] = sel((a[0] - b[1], a[1] + b[0]), v[k])
                        u[z.frames - k] = sel((a[0] + b[1], b[0] - a[1]), v[z.frames - k])
                    v = u
                x = fft(v, 1.0)
                r0 = s * z.ny + qt * SUB
                r1 = z.sc * z.ny + r0
                for n in range(z.frames):
                    out_scr[n // z.f, n % z.f, l, r0 : r0 + SUB, :] = x[n][0]
                    out_scr[n // z.f, n % z.f, l, r1 : r1 + SUB, :] = x[n][1]
    for s in range(z.nx):
        outs[s][:, 0] = out_scr[lax.rem(ip + s, z.nx)]


def kernel4(z, special, idx, arrays):
    out_spec = pl.BlockSpec((z.f, 1, z.lt, z.rows, LANES), lambda i, _: (0, i, 0, 0, 0))
    in_spec = pl.BlockSpec((z.sc, 2, 1, z.lt, z.frames, LANES), lambda i, _: (0, 0, i, 0, 0, 0))
    return pl.pallas_call(
        functools.partial(k4_body, z, special),
        out_shape=[jax.ShapeDtypeStruct((z.f, z.wp, z.lt, z.rows, LANES), F32)] * z.nx,
        grid_spec=pltpu.PrefetchScalarGridSpec(
            num_scalar_prefetch=1,
            grid=(z.wp,),
            in_specs=[in_spec] * z.ny,
            out_specs=[out_spec] * z.nx,
            scratch_shapes=[
                pltpu.VMEM((z.ny, z.sc, 2, z.lt, z.frames, LANES), F32),
                pltpu.VMEM((z.nx, z.f, z.lt, z.rows, LANES), F32),
            ],
        ),
        cost_estimate=pl.CostEstimate(flops=10**9, bytes_accessed=3 * 10**6, transcendentals=0),
        name="k4",
    )(idx, *arrays)


def k3_body(z, special, step_rows, idx_ref, tw_ref, w1_ref, b1_ref, w2_ref, b2_ref, *refs):
    ins, outs = refs[: z.ny], refs[z.ny : 2 * z.ny]
    x_scr, e_scr, t_scr = refs[2 * z.ny :]
    iq = idx_ref[1]
    cl, fr, mm = z.cl, z.frames, z.m
    for s in range(z.ny):
        x_scr[lax.rem(iq + z.ny - s, z.ny)] = ins[s][0]

    def along(sign, load, store):
        def tile(ft, carry):
            rows = pl.ds(pl.multiple_of(ft * SUB, SUB), SUB)
            for l in range(z.lt):
                out = fft([load(m, l, rows) for m in range(mm)], sign)
                for k in range(mm):
                    store(k, l, rows, out[k])
            return carry

        lax.fori_loop(0, fr // SUB, tile, 0)

    lane = lambda l: slice(l * LANES, (l + 1) * LANES)

    def load_x(m, l, rows):
        return tuple(x_scr[m // z.wp, ri, m % z.wp, l, rows, :] for ri in range(2))

    def store_e(k, l, rows, value):
        for ri in range(2):
            e_scr[ri, k, rows, lane(l)] = value[ri]

    along(-1.0, load_x, store_e)

    def combine(k0, carry):
        parts = []
        for e in range(z.wg):
            a, b = (e_scr[ri, k0, :, e * cl : (e + 1) * cl] for ri in range(2))
            if e:
                c, s = tw_ref[0, e * mm + k0], tw_ref[1, e * mm + k0]
                a, b = a * c + b * s, b * c - a * s
            parts.append((a, b))
        for t, value in enumerate(fft(parts, -1.0)):
            rows = pl.ds(pl.multiple_of((k0 + t * mm) * fr, SUB), fr)
            t_scr[0, rows, :] = value[0]
            t_scr[1, rows, :] = value[1]
        return carry

    lax.fori_loop(0, mm, combine, 0)

    def dense(values, w_ref):
        high, low = split_bf16(values)
        wh, wl = w_ref[0], w_ref[1]
        out = dot32(high, wh) + (dot32(low, wh) + dot32(high, wl))
        return out[:, :cl], out[:, cl:]

    def first(rows):
        ar, ai = dense(t_scr[0, rows, :], w1_ref)
        br, bi = dense(t_scr[1, rows, :], w1_ref)
        return ar - bi, ai + br, ar + bi, ai - br

    def second(values):
        out = []
        for real, imag in (values[:2], values[2:]):
            real = jnp.maximum(real + b1_ref[0:1], 0.0)
            imag = jnp.maximum(imag + b1_ref[1:2], 0.0)
            ar, ai = dense(real, w2_ref)
            br, bi = dense(imag, w2_ref)
            for v in (ar - bi + b2_ref[0:1], ai + br + b2_ref[1:2]):
                out.append(jnp.maximum(v - 0.1, 0.0) + jnp.minimum(v + 0.1, 0.0))
        return out

    total = z.w * fr
    row_range = lambda i: pl.ds(pl.multiple_of(i * step_rows, SUB), step_rows)

    if not special:

        def both(i, carry):
            rows = row_range(i)
            out = second(first(rows))
            t_scr[0, rows, :] = out[0] + out[2]
            t_scr[1, rows, :] = out[1] - out[3]
            return carry

        lax.fori_loop(0, total // step_rows, both, 0)
    else:

        def one(i, carry):
            rows = row_range(i)
            for n, v in enumerate(first(rows)):
                t_scr[n, rows, :] = v
            return carry

        def two(i, carry):
            rows = row_range(i)
            for n, v in enumerate(second([t_scr[n, rows, :] for n in range(4)])):
                t_scr[n, rows, :] = v
            return carry

        def three(i, carry):
            rows = row_range(i)
            t_scr[0, rows, :] = t_scr[0, rows, :] + t_scr[2, rows, :]
            t_scr[1, rows, :] = t_scr[1, rows, :] - t_scr[3, rows, :]
            return carry

        lone = jnp.logical_and(iq == 0, pl.program_id(0) == 0)
        sub = lax.broadcasted_iota(jnp.int32, (fr, cl), 0)
        picked = jnp.logical_or(sub == 0, sub == fr // 2)

        def mirror(fix):
            def step(k, carry):
                here = pl.ds(pl.multiple_of(k * fr, SUB), fr)
                there = pl.ds(pl.multiple_of(lax.rem(z.w - k, z.w) * fr, SUB), fr)
                a = [t_scr[n, here, :] for n in range(4)]
                b = [t_scr[n, there, :] for n in range(4)]
                new_a, new_b = fix(a, b), fix(b, a)
                for n in range(4):
                    t_scr[n, here, :] = jnp.where(picked, new_a[n], a[n])
                    t_scr[n, there, :] = jnp.where(picked, new_b[n], b[n])
                return carry

            @pl.when(lone)
            def _():
                lax.fori_loop(0, z.w // 2 + 1, step, 0)

        def apart(a, b):
            return (
                0.5 * (a[0] + b[2]),
                0.5 * (a[1] + b[3]),
                0.5 * (a[1] - b[3]),
                0.5 * (b[2] - a[0]),
            )

        def joined(a, b):
            return (
                a[0] + b[0] - a[3] + b[3],
                a[1] - b[1] + a[2] + b[2],
                jnp.zeros_like(a[0]),
                jnp.zeros_like(a[0]),
            )

        lax.fori_loop(0, total // step_rows, one, 0)
        mirror(apart)
        lax.fori_loop(0, total // step_rows, two, 0)
        mirror(joined)
        lax.fori_loop(0, total // step_rows, three, 0)

    def scatter(k0, carry):
        values = []
        for t in range(z.wg):
            rows = pl.ds(pl.multiple_of((k0 + t * mm) * fr, SUB), fr)
            values.append((t_scr[0, rows, :], t_scr[1, rows, :]))
        sums = fft(values, 1.0)
        pieces = ([], [])
        for e in range(z.wg):
            a, b = sums[e]
            if e:
                c, s = tw_ref[0, e * mm + k0], tw_ref[1, e * mm + k0]
                a, b = a * c - b * s, b * c + a * s
            pieces[0].append(a)
            pieces[1].append(b)
        for ri in range(2):
            if z.lt * LANES > z.wg * cl:
                pieces[ri].append(jnp.zeros((fr, z.lt * LANES - z.wg * cl), F32))
            e_scr[ri, k0] = jnp.concatenate(pieces[ri], axis=1) if len(pieces[ri]) > 1 else pieces[ri][0]
        return carry

    lax.fori_loop(0, mm, scatter, 0)

    def load_e(k, l, rows):
        return tuple(e_scr[ri, k, rows, lane(l)] for ri in range(2))

    def store_x(m, l, rows, value):
        for ri in range(2):
            x_scr[m // z.wp, ri, m % z.wp, l, rows, :] = value[ri]

    along(1.0, load_e, store_x)
    for s in range(z.ny):
        outs[s][0] = x_scr[lax.rem(iq + s, z.ny)]


def kernel3(z, special, idx, twiddle, w1, b1, w2, b2, arrays):
    spec = pl.BlockSpec((1, 2, z.wp, z.lt, z.frames, LANES), lambda i, _: (i, 0, 0, 0, 0, 0))
    const = lambda x: pl.BlockSpec(x.shape, lambda i, _: (0,) * x.ndim)
    total = z.w * z.frames
    step_rows = next(r for r in (128, 64, 32, 16, 8) if total % r == 0)
    return pl.pallas_call(
        functools.partial(k3_body, z, special, step_rows),
        out_shape=[jax.ShapeDtypeStruct((z.sc, 2, z.wp, z.lt, z.frames, LANES), F32)] * z.ny,
        grid_spec=pltpu.PrefetchScalarGridSpec(
            num_scalar_prefetch=1,
            grid=(z.sc,),
            in_specs=[pl.BlockSpec(memory_space=pltpu.SMEM), const(w1), const(b1), const(w2), const(b2)]
            + [spec] * z.ny,
            out_specs=[spec] * z.ny,
            scratch_shapes=[
                pltpu.VMEM((z.ny, 2, z.wp, z.lt, z.frames, LANES), F32),
                pltpu.VMEM((2, z.m, z.frames, z.lt * LANES), F32),
                pltpu.VMEM((4, total, z.cl), F32),
            ],
        ),
        cost_estimate=pl.CostEstimate(flops=4 * 10**9, bytes_accessed=3 * 10**6, transcendentals=0),
        name="k3",
    )(idx, twiddle, w1, b1, w2, b2, *arrays)


def k5_body(z, tile, idx_ref, base_ref, mat_ref, gain_ref, shift_ref, fc1_ref, fb1_ref, fc2_ref, fb2_ref, *refs):
    n_in = z.chunks * z.nx
    ins, out_ref = refs[:n_in], refs[n_in]
    z_scr, after_scr, norm_scr = refs[n_in + 1 :]
    ip = idx_ref[0]
    for c in range(z.chunks):
        for s in range(z.nx):
            p = lax.rem(ip + z.nx - s, z.nx)
            z_scr[p, :, :, c * z.rows : (c + 1) * z.rows, :] = ins[c * z.nx + s][0]
    mat = mat_ref[...]
    for wp in range(z.wp):
        mixed = []
        for p in range(z.nx):
            value = jnp.concatenate([z_scr[p, wp, l] for l in range(z.lt)], axis=1) if z.lt > 1 else z_scr[p, wp, 0]
            mixed.append(dot32(mat, rhs3(value)))
        for e in range(z.wg):
            w = wp * z.wg + e
            rows = slice(w * z.h, (w + 1) * z.h)
            after = base_ref[0, w] + jnp.concatenate([y[:, e * z.cl : (e + 1) * z.cl] for y in mixed], axis=1)
            after_scr[rows, :] = after
            mean = jnp.mean(after, axis=-1, keepdims=True)
            centred = after - mean
            var = jnp.mean(centred * centred, axis=-1, keepdims=True)
            normed = centred / jnp.sqrt(var + 1e-05) * gain_ref[...] + shift_ref[...]
            norm_scr[rows, :] = normed.astype(BF16)
    total = fc1_ref.shape[1]
    after_scr[...] = after_scr[...] + fb2_ref[...]

    def hidden_tile(i, carry):
        cols = pl.ds(pl.multiple_of(i * tile, LANES), tile)
        hidden = dot32(norm_scr[...], fc1_ref[:, cols]) + fb1_ref[:, cols]
        hidden = jax.nn.gelu(hidden).astype(BF16)
        after_scr[...] += dot32(hidden, fc2_ref[cols, :])
        return carry

    lax.fori_loop(0, total // tile, hidden_tile, 0)
    for w in range(z.wl):
        out_ref[0, w] = after_scr[w * z.h : (w + 1) * z.h, :]


def kernel5(z, idx, base, matrix, gain, shift, fc_in, fc_in_bias, fc_out, fc_out_bias, arrays):
    const = lambda x: pl.BlockSpec(x.shape, lambda i, _: (0,) * x.ndim)
    consts = [matrix, gain[None], shift[None], fc_in, fc_in_bias[None], fc_out, fc_out_bias[None]]
    flat = [a for chunk in arrays for a in chunk]
    ff = fc_in.shape[1]
    tile = next(t for t in (768, 512, 384, 256, 128) if ff % t == 0)
    return pl.pallas_call(
        functools.partial(k5_body, z, tile),
        out_shape=jax.ShapeDtypeStruct((z.f, z.wl, z.h, z.c), F32),
        grid_spec=pltpu.PrefetchScalarGridSpec(
            num_scalar_prefetch=1,
            grid=(z.f,),
            in_specs=[pl.BlockSpec((1, z.wl, z.h, z.c), lambda i, _: (i, 0, 0, 0))]
            + [const(x) for x in consts]
            + [pl.BlockSpec((1, z.wp, z.lt, z.rows, LANES), lambda i, _: (i, 0, 0, 0, 0))] * len(flat),
            out_specs=pl.BlockSpec((1, z.wl, z.h, z.c), lambda i, _: (i, 0, 0, 0)),
            scratch_shapes=[
                pltpu.VMEM((z.nx, z.wp, z.lt, z.h, LANES), F32),
                pltpu.VMEM((z.wl * z.h, z.c), F32),
                pltpu.VMEM((z.wl * z.h, z.c), BF16),
            ],
        ),
        cost_estimate=pl.CostEstimate(flops=2 * 10**10, bytes_accessed=3 * 10**7, transcendentals=0),
        name="k5",
    )(idx, base, *consts, *flat)


def exchange(arrays, axis, size):
    out = [arrays[0]]
    for s in range(1, size):
        out.append(lax.ppermute(arrays[s], axis, [(j, (j + s) % size) for j in range(size)]))
    return out


def block_weights(z, weight):
    eye = jnp.eye(z.groups, dtype=F32)
    full = weight[:, :, :, None, :] * eye[None, :, None, :, None]
    full = full.reshape(2, z.groups * z.block, z.groups * z.block)
    high, low = split_outside(jnp.concatenate([full[0], full[1]], axis=1))
    return jnp.stack([high, low])


def body(
    mesh,
    latents,
    norm1_gain,
    norm1_shift,
    spectral_in,
    spectral_in_bias,
    spectral_out,
    spectral_out_bias,
    norm2_gain,
    norm2_shift,
    fc_in,
    fc_in_bias,
    fc_out,
    fc_out_bias,
):
    z = Sizes(mesh, latents.shape, spectral_in.shape)
    idx = jnp.stack([lax.axis_index("px"), lax.axis_index("py")]).astype(jnp.int32)
    forward, inverse = height_tables(z)
    angle = 2.0 * math.pi * np.outer(np.arange(z.wg), np.arange(z.m)) / z.w
    twiddle = jnp.asarray(np.stack([np.cos(angle).ravel(), np.sin(angle).ravel()]).astype(np.float32))
    w1, w2 = block_weights(z, spectral_in), block_weights(z, spectral_out)
    b1, b2 = spectral_in_bias.reshape(2, z.cl), spectral_out_bias.reshape(2, z.cl)

    turned = jnp.transpose(latents, (0, 2, 1, 3))
    base, sent = kernel1(z, idx, turned, norm1_gain, norm1_shift, jnp.asarray(stacked3(forward)))
    returned = []
    for c in range(z.chunks):
        special = c == 0
        held = exchange(sent[c], "px", z.nx)
        held = exchange(kernel2(z, special, idx, held), "py", z.ny)
        held = exchange(kernel3(z, special, idx, twiddle, w1, b1, w2, b2, held), "py", z.ny)
        returned.append(exchange(kernel4(z, special, idx, held), "px", z.nx))
    result = kernel5(
        z,
        idx,
        base,
        jnp.asarray(stacked3(inverse)),
        norm2_gain,
        norm2_shift,
        fc_in,
        fc_in_bias,
        fc_out,
        fc_out_bias,
        returned,
    )
    return jnp.transpose(result, (0, 2, 1, 3))


def solution(mesh):
    return jax.shard_map(
        functools.partial(body, mesh),
        mesh=mesh,
        in_specs=(
            P("px", None, "py", None),
            P(),
            P(),
            P(None, "px", None, None),
            P(None, "px", None),
            P(None, "px", None, None),
            P(None, "px", None),
            P(),
            P(),
            P(),
            P(),
            P(),
            P(),
        ),
        out_specs=P("px", None, "py", None),
        check_vma=False,
    )
```
